256 devices in a mesh: group: 8 (over z), shard: 32 (over x, y, core).
Axes of the slice: x: 4, y: 4, z: 8, core: 2. Of those that a mesh axis runs over, the one named last changes fastest.
Arguments:
- queries: bfloat16 [1536, 1024], P(('group', 'shard')), may hold values from -12 to 12
- candidates: bfloat16 [1048576, 1024], P(('group', 'shard')), may hold values from -4 to 4
- targets: int32 [1536], replicated, may hold values from 0 to 1048575
Outputs:
- losses: float32 [1536], replicated
- mean_loss: float32 [], replicated
The draws below stay inside these ranges and needn't reach their ends.
All inputs are finite; a program needn't handle non-finite values.
Results may differ from the reference program's by a relative error of at most 0.0003.
Values may be sent and summed in bfloat16 or wider, within the bound.
No kernel may reach another device: no remote copies, remote signals or barrier semaphores. Data moves between devices by JAX's collectives and lax.ppermute only.
A program may use at most 64 MiB of HBM per device.

```python
import jax
import jax.numpy as jnp
from jax import lax

D = 1024
CAND_DEV = 4096
QUERIES = 1536
CANDS = 1048576
N_GROUP = 8
N_SHARD = 32


def shared_queries(key):
    normal_key = jax.random.fold_in(key, 11)
    base = jnp.clip(jax.random.normal(normal_key, (QUERIES, D), jnp.float32), -6.0, 6.0)
    return base


def draw_queries(key, part):
    base = shared_queries(key)
    return base.astype(jnp.bfloat16)


def draw_candidates(key, part):
    cand_key = jax.random.fold_in(key, 21)
    size_key = jax.random.fold_in(key, 22)
    order_key = jax.random.fold_in(key, 31)
    offset_key = jax.random.fold_in(key, 32)
    height_key = jax.random.fold_in(key, 33)
    row_sizes = 0.5 * jnp.exp(jax.random.uniform(size_key, (CANDS, 1), jnp.float32, 0.0, 1.0) * jnp.log(8.0))
    rows = jnp.clip(jax.random.normal(cand_key, (CANDS, D), jnp.float32), -6.0, 6.0)
    rows = rows * row_sizes * D ** (-0.5)
    base = shared_queries(key)
    plant_norms = 0.5 * jnp.exp(jax.random.uniform(height_key, (QUERIES,), jnp.float32, 0.0, 1.0) * jnp.log(8.0))
    heights = plant_norms * D ** (-0.5)
    strong = jnp.arange(QUERIES, dtype=jnp.int32) < 8
    heights = jnp.where(strong, jnp.float32(min(4.0, 300.0 / D)), heights)
    aligned = jnp.where(base >= 0.0, heights[:, None], -heights[:, None])
    stride = CANDS // QUERIES
    order = jax.random.permutation(order_key, QUERIES).astype(jnp.int32)
    offsets = jax.random.randint(offset_key, (QUERIES,), 0, stride, jnp.int32)
    places = order * stride + offsets
    rows = rows.at[places].set(aligned)
    return rows.astype(jnp.bfloat16)


def plant(values, own_key, least, top_value):
    index_at = [jax.random.randint(jax.random.fold_in(own_key, axis), (), 0, length) for axis, length in enumerate(values.shape)]
    widest = values.shape.index(max(values.shape))
    beside = index_at[:widest] + [(index_at[widest] + 1) % values.shape[widest]] + index_at[widest + 1:]
    return values.at[tuple(index_at)].set(least).at[tuple(beside)].set(top_value)


def setup_inputs(seed: int = 0) -> dict:
    arg_keys = jax.random.split(jax.random.key(seed), 4)
    queries = draw_queries(jax.random.fold_in(arg_keys[3], 71), 0)
    candidates = draw_candidates(jax.random.fold_in(arg_keys[3], 71), 0)
    targets = plant(jax.random.randint(arg_keys[2], (QUERIES,), 0, CANDS), jax.random.fold_in(arg_keys[2], 1), 0, CANDS - 1).astype(jnp.int32)
    return dict(queries=queries, candidates=candidates, targets=targets)


def reference(queries, candidates, targets):
    blocks = candidates.reshape(N_GROUP * N_SHARD, CAND_DEV, D)

    def step(carry, block):
        top, total = carry
        scores = jnp.dot(queries, block.T, preferred_element_type=jnp.float32)
        block_top = jnp.max(scores, axis=1)
        new_top = jnp.maximum(top, block_top)
        total = total * jnp.exp(top - new_top) + jnp.sum(jnp.exp(scores - new_top[:, None]), axis=1)
        return (new_top, total), None

    start = (jnp.full((QUERIES,), -jnp.inf, jnp.float32), jnp.zeros((QUERIES,), jnp.float32))
    (top, total), unused = lax.scan(step, start, blocks)
    chosen = jnp.take(candidates, targets.astype(jnp.int32), axis=0)
    picked = jnp.sum(queries.astype(jnp.float32) * chosen.astype(jnp.float32), axis=1)
    losses = top + jnp.log(total) - picked
    return losses, jnp.mean(losses)
```

```python
import functools

import jax
import jax.numpy as jnp
from jax import lax
from jax.experimental import pallas as pl
from jax.experimental.pallas import tpu as pltpu
from jax.sharding import Mesh
from jax.sharding import PartitionSpec as P

SHARD = ("x", "y", "core")
EVERY = ("group", *SHARD)
TILE = 512


def broadcast_to_peers(value, axis):
    copies = jnp.broadcast_to(value, (lax.axis_size(axis), *value.shape))
    return lax.all_to_all(copies, axis, split_axis=0, concat_axis=0, tiled=True)


def shifted(value, axis, step):
    size = lax.axis_size(axis)
    return lax.ppermute(value, axis, [(k, (k + step) % size) for k in range(size)])


def score_kernel(tile, queries, candidates, targets, out, scores):
    rows, count = candidates.shape[0], queries.shape[0]
    blocks, groups = rows // tile, tile // 8
    offset = targets[...] - lax.broadcasted_iota(jnp.int32, (8, count), 0)

    def multiply(block, slot):
        part = candidates[pl.ds(pl.multiple_of(block * tile, tile), tile), :]
        scores[slot] = lax.dot_general(
            part, queries[...], (((1,), (1,)), ((), ())), preferred_element_type=jnp.float32
        )

    def fold(block, slot, carry):
        top, total, picked = carry
        here = scores[slot].reshape(groups, 8, count)
        peak = jnp.maximum(top, jnp.max(here, axis=0))
        total = total * jnp.exp(top - peak) + jnp.sum(jnp.exp(here - peak[None]), axis=0)
        local = offset - block * tile
        for k in range(groups):
            picked = jnp.where(local == 8 * k, here[k], picked)
        return peak, total, picked

    def pair(step, carry):
        block = 2 * step
        multiply(block + 1, 1)
        carry = fold(block, 0, carry)
        multiply(block + 2, 0)
        return fold(block + 1, 1, carry)

    zero = jnp.zeros((8, count), jnp.float32)
    carry = (jnp.full((8, count), -jnp.inf, jnp.float32), zero, zero)
    multiply(0, 0)
    carry = lax.fori_loop(0, blocks // 2 - 1, pair, carry)
    multiply(blocks - 1, 1)
    carry = fold(blocks - 2, 0, carry)
    top, total, picked = fold(blocks - 1, 1, carry)
    peak = jnp.max(top, axis=0, keepdims=True)
    total = jnp.sum(total * jnp.exp(top - peak), axis=0, keepdims=True)
    out[0:1, :] = peak + jnp.log(total)
    out[1:2, :] = jnp.sum(picked, axis=0, keepdims=True)


def score(queries, candidates, targets):
    count, width = queries.shape
    rows = candidates.shape[0]
    return pl.pallas_call(
        functools.partial(score_kernel, TILE),
        out_shape=jax.ShapeDtypeStruct((2, count), jnp.float32),
        in_specs=[pl.BlockSpec(memory_space=pltpu.VMEM)] * 3,
        out_specs=pl.BlockSpec(memory_space=pltpu.VMEM),
        scratch_shapes=[pltpu.VMEM((2, TILE, count), jnp.float32)],
        compiler_params=pltpu.CompilerParams(vmem_limit_bytes=16 * 2**20),
        cost_estimate=pl.CostEstimate(
            flops=2 * count * rows * width,
            bytes_accessed=2 * width * (count + rows),
            transcendentals=count * rows,
        ),
        name="score",
    )(queries, candidates, targets.reshape(1, count))


def merge(parts):
    lse, picked = parts[:, 0], parts[:, 1]
    top = jnp.max(lse, axis=0)
    lse = top + jnp.log(jnp.sum(jnp.exp(lse - top), axis=0))
    return jnp.stack([lse, jnp.sum(picked, axis=0)])


def on_device(queries, candidates, targets):
    rows, width = candidates.shape
    at = {axis: lax.axis_index(axis) for axis in EVERY}
    sizes = [lax.axis_size(axis) for axis in EVERY]
    groups, xs, ys, cores = sizes
    each = queries.shape[0]
    owner = 0
    for axis, size in zip(EVERY, sizes):
        owner = owner * size + at[axis]
    local = targets - owner * rows
    local = local.reshape(*sizes, each).transpose(2, 3, 1, 0, 4).reshape(ys, -1)

    line = broadcast_to_peers(queries, "group").reshape(-1, width)
    plane = jnp.zeros((xs, *line.shape), line.dtype)
    plane = lax.dynamic_update_index_in_dim(plane, line, at["x"], 0)
    for step, piece in [(k, shifted(line, "x", k)) for k in (1, xs - 1, 2)]:
        plane = lax.dynamic_update_index_in_dim(plane, piece, (at["x"] - step) % xs, 0)
    plane = plane.reshape(-1, width)

    found = jnp.zeros((ys, 2, cores * plane.shape[0]), jnp.float32)
    steps = (0, 1, ys - 1, 2)
    mine = [plane, *(shifted(plane, "y", k) for k in steps[1:])]
    for step, block in zip(steps, mine):
        other = shifted(block, "core", 1)
        first = jnp.where(at["core"] == 0, block, other)
        second = jnp.where(at["core"] == 0, other, block)
        place = (at["y"] - step) % ys
        chosen = lax.dynamic_index_in_dim(local, place, 0, keepdims=False)
        result = score(jnp.concatenate([first, second]), candidates, chosen)
        found = lax.dynamic_update_index_in_dim(found, result, place, 0)

    partial = found.transpose(1, 0, 2).reshape(2, -1)
    partial = merge(jnp.stack([partial, shifted(partial, "core", 1)]))
    partial = merge(broadcast_to_peers(partial, ("x", "y")))
    lse, picked = merge(broadcast_to_peers(partial, "group"))
    losses = lse - picked
    losses = losses.reshape(ys, cores, xs, groups, each).transpose(3, 2, 0, 1, 4).reshape(-1)
    return (losses, jnp.mean(losses))


def solution(mesh):
    finer = Mesh(mesh.devices.reshape(mesh.shape["group"], 4, 4, 2), EVERY)
    in_specs = (P(EVERY, None), P(EVERY, None), P())
    out_specs = (P(), P())
    return jax.shard_map(
        on_device, mesh=finer, in_specs=in_specs, out_specs=out_specs, check_vma=False
    )
```

```python
import functools

import jax
import jax.numpy as jnp
from jax import lax
from jax.experimental import pallas as pl
from jax.experimental.pallas import tpu as pltpu
from jax.sharding import Mesh
from jax.sharding import PartitionSpec as P

SHARD = ("x", "y", "core")
EVERY = ("group", *SHARD)
TILE = 512


def broadcast_to_peers(value, axis):
    copies = jnp.broadcast_to(value, (lax.axis_size(axis), *value.shape))
    return lax.all_to_all(copies, axis, split_axis=0, concat_axis=0, tiled=True)


def shifted(value, axis, step):
    size = lax.axis_size(axis)
    return lax.ppermute(value, axis, [(k, (k + step) % size) for k in range(size)])


def turned(axis):
    size = lax.axis_size(axis)
    at = lax.axis_index(axis).astype(jnp.uint32)
    return [lax.rem(at + jnp.uint32(size - k), jnp.uint32(size)) for k in range(size)]


def score_kernel(tiles, queries, candidates, targets, out, scores, *stream):
    count = queries.shape[0]
    starts = [sum(tiles[:k]) for k in range(len(tiles))]
    places = [pl.ds(start, tile) for start, tile in zip(starts, tiles)]
    local = targets[...] - lax.broadcasted_iota(jnp.int32, (8, count), 0)
    source, copies = candidates, {}
    if stream:
        source, sems = stream
        cuts = [0, starts[1], starts[len(tiles) // 2], candidates.shape[0]]
        for k, (start, end) in enumerate(zip(cuts, cuts[1:])):
            part = pl.ds(start, end - start)
            copy = pltpu.make_async_copy(candidates.at[part], source.at[part], sems.at[k])
            copy.start()
            copies[starts.index(start)] = copy

    def multiply(k):
        if k in copies:
            copies[k].wait()
        scores[k % 2, : tiles[k]] = lax.dot_general(
            source[places[k], :],
            queries[...],
            (((1,), (1,)), ((), ())),
            preferred_element_type=jnp.float32,
        )

    top = jnp.full((8, count), -jnp.inf, jnp.float32)
    total = picked = jnp.zeros((8, count), jnp.float32)
    multiply(0)
    for k, tile in enumerate(tiles):
        if k + 1 < len(tiles):
            multiply(k + 1)
        here = scores[k % 2, :tile].reshape(tile // 8, 8, count)
        peak = jnp.maximum(top, jnp.max(here, axis=0))
        total = total * jnp.exp(top - peak) + jnp.sum(jnp.exp(here - peak[None]), axis=0)
        top = peak
        for row in range(tile // 8):
            picked = jnp.where(local == starts[k] + 8 * row, here[row], picked)
    peak = jnp.max(top, axis=0, keepdims=True)
    total = jnp.sum(total * jnp.exp(top - peak), axis=0, keepdims=True)
    out[0:1, :] = peak + jnp.log(total)
    out[1:2, :] = jnp.sum(picked, axis=0, keepdims=True)


def score(queries, candidates, targets, streamed=False):
    count, width = queries.shape
    rows = candidates.shape[0]
    tiles = [TILE // 2] + [TILE] * (rows // TILE - 1) + [TILE // 2]
    scratch = [pltpu.VMEM((2, TILE, count), jnp.float32)]
    if streamed:
        scratch += [
            pltpu.VMEM(candidates.shape, candidates.dtype),
            pltpu.SemaphoreType.DMA((3,)),
        ]
    vmem = pl.BlockSpec(memory_space=pltpu.VMEM)
    return pl.pallas_call(
        functools.partial(score_kernel, tiles),
        out_shape=jax.ShapeDtypeStruct((2, count), jnp.float32),
        in_specs=[vmem, pl.BlockSpec(memory_space=pl.ANY) if streamed else vmem, vmem],
        out_specs=vmem,
        scratch_shapes=scratch,
        compiler_params=pltpu.CompilerParams(
            vmem_limit_bytes=(50 if streamed else 16) * 2**20
        ),
        cost_estimate=pl.CostEstimate(
            flops=2 * count * rows * width,
            bytes_accessed=2 * width * (count + rows),
            transcendentals=count * rows,
        ),
        name="score",
    )(queries, candidates, targets)


def merge(parts):
    lse, picked = parts[:, 0], parts[:, 1]
    top = jnp.max(lse, axis=0)
    lse = top + jnp.log(jnp.sum(jnp.exp(lse - top), axis=0))
    return jnp.stack([lse, jnp.sum(picked, axis=0)])


def on_device(queries, candidates, targets):
    rows, width = candidates.shape
    at = {axis: lax.axis_index(axis) for axis in EVERY}
    sizes = [lax.axis_size(axis) for axis in EVERY]
    groups, xs, ys, cores = sizes
    each = queries.shape[0]
    owner = 0
    for axis, size in zip(EVERY, sizes):
        owner = owner * size + at[axis]

    local = targets - owner * rows
    local = local.reshape(*sizes, each).transpose(2, 3, 1, 0, 4).reshape(ys, -1)
    x_place = turned("x")
    y_place = turned("y")
    line = broadcast_to_peers(queries, "group").reshape(-1, width)
    line, local, x_place, y_place, even = lax.optimization_barrier(
        (line, local, x_place, y_place, at["core"] == 0)
    )
    pieces = [(k, shifted(line, "x", k)) for k in (1, xs - 1, 2)]
    plane = jnp.zeros((xs, *line.shape), line.dtype)
    plane = lax.dynamic_update_index_in_dim(plane, line, x_place[0], 0)
    for step, piece in pieces:
        plane = lax.dynamic_update_index_in_dim(plane, piece, x_place[step], 0)
    plane = plane.reshape(-1, width)
    chosen = [lax.dynamic_slice_in_dim(local, place, 1, 0) for place in y_place]

    def chip(block):
        other = shifted(block, "core", 1)
        return jnp.concatenate([jnp.where(even, block, other), jnp.where(even, other, block)])

    near = [shifted(plane, "y", k) for k in (1, ys - 1)]
    mine = score(chip(plane), candidates, chosen[0], True)
    half = plane.shape[0] // 2
    far = [shifted(near[0][:half], "y", 1), shifted(near[1][half:], "y", ys - 1)]
    beside = score(
        jnp.concatenate([chip(block) for block in near]),
        candidates,
        jnp.concatenate([chosen[1], chosen[3]], axis=1),
    )
    last = score(chip(jnp.concatenate(far)), candidates, chosen[2])

    mine, beside, last = lax.optimization_barrier((mine, beside, last))
    found = jnp.zeros((2, ys, last.shape[1]), jnp.float32)
    parts = [(0, mine), (1, beside[:, : last.shape[1]]), (ys - 1, beside[:, last.shape[1] :]), (2, last)]
    for step, part in parts:
        found = lax.dynamic_update_index_in_dim(found, part, y_place[step], 1)
    partial = found.reshape(2, -1)
    partial = merge(jnp.stack([partial, shifted(partial, "core", 1)]))
    partial = merge(broadcast_to_peers(partial, ("x", "y")))
    lse, picked = merge(broadcast_to_peers(partial, "group"))
    losses = lse - picked
    losses = losses.reshape(ys, cores, xs, groups, each).transpose(3, 2, 0, 1, 4).reshape(-1)
    return (losses, jnp.mean(losses))


def solution(mesh):
    finer = Mesh(mesh.devices.reshape(mesh.shape["group"], 4, 4, 2), EVERY)
    in_specs = (P(EVERY, None), P(EVERY, None), P())
    out_specs = (P(), P())
    return jax.shard_map(
        on_device, mesh=finer, in_specs=in_specs, out_specs=out_specs, check_vma=False
    )
```

```python
import functools

import jax
import jax.numpy as jnp
from jax import lax
from jax.experimental import pallas as pl
from jax.experimental.pallas import tpu as pltpu
from jax.sharding import Mesh
from jax.sharding import PartitionSpec as P

SHARD = ("x", "y", "core")
EVERY = ("group", *SHARD)
TILE = 512


def broadcast_to_peers(value, axis):
    copies = jnp.broadcast_to(value, (lax.axis_size(axis), *value.shape))
    return lax.all_to_all(copies, axis, split_axis=0, concat_axis=0, tiled=True)


def shifted(value, axis, step):
    size = lax.axis_size(axis)
    return lax.ppermute(value, axis, [(k, (k + step) % size) for k in range(size)])


def turned(axis):
    size = lax.axis_size(axis)
    at = lax.axis_index(axis).astype(jnp.uint32)
    return [lax.rem(at + jnp.uint32(size - k), jnp.uint32(size)) for k in range(size)]


def score_kernel(tiles, queries, candidates, targets, out, scores, *stream):
    count = queries.shape[0]
    starts = [sum(tiles[:k]) for k in range(len(tiles))]
    places = [pl.ds(start, tile) for start, tile in zip(starts, tiles)]
    local = targets[...] - lax.broadcasted_iota(jnp.int32, (8, count), 0)
    source, copies = candidates, {}
    if stream:
        source, sems = stream
        cuts = [0, starts[1], starts[len(tiles) // 2], candidates.shape[0]]
        for k, (start, end) in enumerate(zip(cuts, cuts[1:])):
            part = pl.ds(start, end - start)
            copy = pltpu.make_async_copy(candidates.at[part], source.at[part], sems.at[k])
            copy.start()
            copies[starts.index(start)] = copy

    def multiply(k):
        if k in copies:
            copies[k].wait()
        scores[k % 2, : tiles[k]] = lax.dot_general(
            source[places[k], :],
            queries[...],
            (((1,), (1,)), ((), ())),
            preferred_element_type=jnp.float32,
        )

    top = jnp.full((8, count), -jnp.inf, jnp.float32)
    total = picked = jnp.zeros((8, count), jnp.float32)
    multiply(0)
    for k, tile in enumerate(tiles):
        if k + 1 < len(tiles):
            multiply(k + 1)
        here = scores[k % 2, :tile].reshape(tile // 8, 8, count)
        peak = jnp.maximum(top, jnp.max(here, axis=0))
        total = total * jnp.exp(top - peak) + jnp.sum(jnp.exp(here - peak[None]), axis=0)
        top = peak
        for row in range(tile // 8):
            picked = jnp.where(local == starts[k] + 8 * row, here[row], picked)
    peak = jnp.max(top, axis=0, keepdims=True)
    total = jnp.sum(total * jnp.exp(top - peak), axis=0, keepdims=True)
    out[0:1, :] = peak + jnp.log(total)
    out[1:2, :] = jnp.sum(picked, axis=0, keepdims=True)


def score(queries, candidates, targets, streamed=False):
    count, width = queries.shape
    rows = candidates.shape[0]
    tiles = [TILE // 2] + [TILE] * (rows // TILE - 1) + [TILE // 2]
    scratch = [pltpu.VMEM((2, TILE, count), jnp.float32)]
    if streamed:
        scratch += [
            pltpu.VMEM(candidates.shape, candidates.dtype),
            pltpu.SemaphoreType.DMA((3,)),
        ]
    vmem = pl.BlockSpec(memory_space=pltpu.VMEM)
    return pl.pallas_call(
        functools.partial(score_kernel, tiles),
        out_shape=jax.ShapeDtypeStruct((2, count), jnp.float32),
        in_specs=[vmem, pl.BlockSpec(memory_space=pl.ANY) if streamed else vmem, vmem],
        out_specs=vmem,
        scratch_shapes=scratch,
        compiler_params=pltpu.CompilerParams(
            vmem_limit_bytes=(50 if streamed else 16) * 2**20
        ),
        cost_estimate=pl.CostEstimate(
            flops=2 * count * rows * width,
            bytes_accessed=2 * width * (count + rows),
            transcendentals=count * rows,
        ),
        name="score",
    )(queries, candidates, targets)


def merge(parts):
    lse, picked = parts[:, 0], parts[:, 1]
    top = jnp.max(lse, axis=0)
    lse = top + jnp.log(jnp.sum(jnp.exp(lse - top), axis=0))
    return jnp.stack([lse, jnp.sum(picked, axis=0)])


def on_device(queries, candidates, targets):
    rows, width = candidates.shape
    at = {axis: lax.axis_index(axis) for axis in EVERY}
    sizes = [lax.axis_size(axis) for axis in EVERY]
    groups, xs, ys, cores = sizes
    each = queries.shape[0]
    owner = 0
    for axis, size in zip(EVERY, sizes):
        owner = owner * size + at[axis]
    base = owner * rows

    x_place = turned("x")
    y_place = turned("y")
    queries, base, x_place, y_place, even = lax.optimization_barrier(
        (queries, base, x_place, y_place, at["core"] == 0)
    )
    line = broadcast_to_peers(queries, "group").reshape(-1, width)
    line, targets = lax.optimization_barrier((line, targets))
    pieces = [(k, shifted(line, "x", k)) for k in (1, xs - 1, 2)]
    local = targets - base
    local = local.reshape(*sizes, each).transpose(2, 3, 1, 0, 4).reshape(ys, -1)
    order = jnp.concatenate(
        [lax.dynamic_slice_in_dim(local, y_place[k], 1, 0) for k in (0, 1, ys - 1, 2)], axis=1
    )
    count = local.shape[1]
    cuts = (0, count * 2 // 3, 2 * count, 2 * count + count * 2 // 3, 4 * count)
    wanted = [order[:, start:end] for start, end in zip(cuts, cuts[1:])]
    plane = jnp.zeros((xs, *line.shape), line.dtype)
    plane = lax.dynamic_update_index_in_dim(plane, line, x_place[0], 0)
    for step, piece in pieces:
        plane = lax.dynamic_update_index_in_dim(plane, piece, x_place[step], 0)
    plane, wanted = lax.optimization_barrier((plane.reshape(-1, width), wanted))

    def chip(block):
        other = shifted(block, "core", 1)
        return jnp.concatenate([jnp.where(even, block, other), jnp.where(even, other, block)])

    near = [shifted(plane, "y", k) for k in (1, ys - 1)]
    own = chip(plane)
    mine = score(own[: cuts[1]], candidates, wanted[0], True)
    half = plane.shape[0] // 2
    far = [shifted(near[0][:half], "y", 1), shifted(near[1][half:], "y", ys - 1)]
    near = [chip(block) for block in near]
    block = jnp.concatenate([own[cuts[1] :], near[0]])
    beside = score(block, candidates, wanted[1])
    rest = score(near[1][: cuts[1]], candidates, wanted[2])
    block = jnp.concatenate([near[1][cuts[1] :], chip(jnp.concatenate(far))])
    last = score(block, candidates, wanted[3])

    parts = lax.optimization_barrier((mine, beside, rest, last))
    parts = jnp.concatenate(parts, axis=1).reshape(2, ys, count)
    found = jnp.zeros_like(parts)
    for place, step in enumerate((0, 1, ys - 1, 2)):
        found = lax.dynamic_update_index_in_dim(found, parts[:, place], y_place[step], 1)
    partial = found.reshape(2, -1)
    partial = merge(jnp.stack([partial, shifted(partial, "core", 1)]))
    partial = merge(broadcast_to_peers(partial, ("x", "y")))
    lse, picked = merge(broadcast_to_peers(partial, "group"))
    losses = lse - picked
    losses = losses.reshape(ys, cores, xs, groups, each).transpose(3, 2, 0, 1, 4).reshape(-1)
    return (losses, jnp.mean(losses))


def solution(mesh):
    finer = Mesh(mesh.devices.reshape(mesh.shape["group"], 4, 4, 2), EVERY)
    in_specs = (P(EVERY, None), P(EVERY, None), P())
    out_specs = (P(), P())
    return jax.shard_map(
        on_device, mesh=finer, in_specs=in_specs, out_specs=out_specs, check_vma=False
    )
```

```python
import functools

import jax
import jax.numpy as jnp
from jax import lax
from jax.experimental import pallas as pl
from jax.experimental.pallas import tpu as pltpu
from jax.sharding import Mesh
from jax.sharding import PartitionSpec as P

SHARD = ("x", "y", "core")
EVERY = ("group", *SHARD)
TILE = 512


def broadcast_to_peers(value, axis):
    copies = jnp.broadcast_to(value, (lax.axis_size(axis), *value.shape))
    return lax.all_to_all(copies, axis, split_axis=0, concat_axis=0, tiled=True)


def shifted(value, axis, step):
    size = lax.axis_size(axis)
    return lax.ppermute(value, axis, [(k, (k + step) % size) for k in range(size)])


def forwarded(value):
    ys, cores = lax.axis_size("y"), lax.axis_size("core")
    pairs = [
        (y * cores + core, (y + (1, ys - 1)[core]) % ys * cores + core)
        for y in range(ys)
        for core in range(cores)
    ]
    return lax.ppermute(value, ("y", "core"), pairs)


def turned(axis):
    size = lax.axis_size(axis)
    at = lax.axis_index(axis).astype(jnp.uint32)
    return [lax.rem(at + jnp.uint32(size - k), jnp.uint32(size)) for k in range(size)]


def score_kernel(tiles, queries, candidates, targets, out, scores, *stream):
    count = queries.shape[0]
    starts = [sum(tiles[:k]) for k in range(len(tiles))]
    places = [pl.ds(start, tile) for start, tile in zip(starts, tiles)]
    local = targets[...] - lax.broadcasted_iota(jnp.int32, (8, count), 0)
    source, copies = candidates, {}
    if stream:
        source, sems = stream
        cuts = [0, starts[1], starts[len(tiles) // 2], candidates.shape[0]]
        for k, (start, end) in enumerate(zip(cuts, cuts[1:])):
            part = pl.ds(start, end - start)
            copy = pltpu.make_async_copy(candidates.at[part], source.at[part], sems.at[k])
            copy.start()
            copies[starts.index(start)] = copy

    def multiply(k):
        if k in copies:
            copies[k].wait()
        scores[k % 2, : tiles[k]] = lax.dot_general(
            source[places[k], :],
            queries[...],
            (((1,), (1,)), ((), ())),
            preferred_element_type=jnp.float32,
        )

    top = jnp.full((8, count), -jnp.inf, jnp.float32)
    total = picked = jnp.zeros((8, count), jnp.float32)
    multiply(0)
    for k, tile in enumerate(tiles):
        if k + 1 < len(tiles):
            multiply(k + 1)
        here = scores[k % 2, :tile].reshape(tile // 8, 8, count)
        peak = jnp.maximum(top, jnp.max(here, axis=0))
        total = total * jnp.exp(top - peak) + jnp.sum(jnp.exp(here - peak[None]), axis=0)
        top = peak
        for row in range(tile // 8):
            picked = jnp.where(local == starts[k] + 8 * row, here[row], picked)
    peak = jnp.max(top, axis=0, keepdims=True)
    total = jnp.sum(total * jnp.exp(top - peak), axis=0, keepdims=True)
    out[0:1, :] = peak + jnp.log(total)
    out[1:2, :] = jnp.sum(picked, axis=0, keepdims=True)


def score(queries, candidates, targets, streamed=False):
    count, width = queries.shape
    rows = candidates.shape[0]
    tiles = [TILE // 2] + [TILE] * (rows // TILE - 1) + [TILE // 2]
    scratch = [pltpu.VMEM((2, TILE, count), jnp.float32)]
    if streamed:
        scratch += [
            pltpu.VMEM(candidates.shape, candidates.dtype),
            pltpu.SemaphoreType.DMA((3,)),
        ]
    vmem = pl.BlockSpec(memory_space=pltpu.VMEM)
    return pl.pallas_call(
        functools.partial(score_kernel, tiles),
        out_shape=jax.ShapeDtypeStruct((2, count), jnp.float32),
        in_specs=[vmem, pl.BlockSpec(memory_space=pl.ANY) if streamed else vmem, vmem],
        out_specs=vmem,
        scratch_shapes=scratch,
        compiler_params=pltpu.CompilerParams(
            vmem_limit_bytes=(50 if streamed else 16) * 2**20
        ),
        cost_estimate=pl.CostEstimate(
            flops=2 * count * rows * width,
            bytes_accessed=2 * width * (count + rows),
            transcendentals=count * rows,
        ),
        name="score",
    )(queries, candidates, targets)


def pick_kernel(first_wanted, first, second, out):
    @pl.when(first_wanted[0] == 1)
    def _():
        out[...] = first[...]

    @pl.when(first_wanted[0] == 0)
    def _():
        out[...] = second[...]


def picked_block(first_wanted, first, second):
    vmem = pl.BlockSpec(memory_space=pltpu.VMEM)
    return pl.pallas_call(
        pick_kernel,
        out_shape=jax.ShapeDtypeStruct(first.shape, first.dtype),
        in_specs=[pl.BlockSpec(memory_space=pltpu.SMEM), vmem, vmem],
        out_specs=vmem,
        compiler_params=pltpu.CompilerParams(vmem_limit_bytes=4 * 2**20),
        cost_estimate=pl.CostEstimate(
            flops=10**6, bytes_accessed=4 * first.size, transcendentals=0
        ),
        name="pick",
    )(first_wanted, first, second)


def prep_kernel(value, out):
    out[...] = value[...]


def prepared(value):
    vmem = pl.BlockSpec(memory_space=pltpu.VMEM)
    return pl.pallas_call(
        prep_kernel,
        out_shape=jax.ShapeDtypeStruct(value.shape, value.dtype),
        in_specs=[vmem],
        out_specs=vmem,
        compiler_params=pltpu.CompilerParams(vmem_limit_bytes=2**20),
        cost_estimate=pl.CostEstimate(flops=2 * 10**10, bytes_accessed=4096, transcendentals=0),
        name="prep",
    )(value)


def merge(parts):
    lse, picked = parts[:, 0], parts[:, 1]
    top = jnp.max(lse, axis=0)
    lse = top + jnp.log(jnp.sum(jnp.exp(lse - top), axis=0))
    return jnp.stack([lse, jnp.sum(picked, axis=0)])


def on_device(queries, candidates, targets):
    rows, width = candidates.shape
    at = {axis: lax.axis_index(axis) for axis in EVERY}
    sizes = [lax.axis_size(axis) for axis in EVERY]
    groups, xs, ys, cores = sizes
    each = queries.shape[0]
    owner = 0
    for axis, size in zip(EVERY, sizes):
        owner = owner * size + at[axis]
    base = owner * rows

    x_place = turned("x")
    y_place = turned("y")
    first_wanted = (at["core"] == 0).astype(jnp.int32).reshape(1)
    queries, base, x_place, y_place, even, first_wanted = lax.optimization_barrier(
        (queries, base, x_place, y_place, at["core"] == 0, first_wanted)
    )
    line = broadcast_to_peers(queries, "group").reshape(-1, width)
    line, targets = lax.optimization_barrier((line, targets))
    pieces = [(k, shifted(line, "x", k)) for k in (1, xs - 1, 2)]
    local = targets - base
    local = local.reshape(*sizes, each).transpose(2, 3, 1, 0, 4).reshape(ys, -1)
    order = jnp.concatenate(
        [lax.dynamic_slice_in_dim(local, y_place[k], 1, 0) for k in (0, 1, ys - 1, 2)], axis=1
    )
    count = local.shape[1]
    cuts = (0, count * 2 // 3, 2 * count, 2 * count + count * 2 // 3, 4 * count)
    wanted = [order[:, start:end] for start, end in zip(cuts, cuts[1:])]
    plane = jnp.zeros((xs, *line.shape), line.dtype)
    plane = lax.dynamic_update_index_in_dim(plane, line, x_place[0], 0)
    for step, piece in pieces:
        plane = lax.dynamic_update_index_in_dim(plane, piece, x_place[step], 0)
    plane, wanted = lax.optimization_barrier((plane.reshape(-1, width), wanted))

    def chip(block):
        other = shifted(block, "core", 1)
        return jnp.concatenate([jnp.where(even, block, other), jnp.where(even, other, block)])

    near = [shifted(plane, "y", k) for k in (1, ys - 1)]
    own = chip(plane)
    mine = score(own[: cuts[1]], candidates, prepared(wanted[0]))
    far = forwarded(picked_block(first_wanted, *near))
    near = [chip(block) for block in near]
    block = jnp.concatenate([own[cuts[1] :], near[0]])
    beside = score(block, candidates, wanted[1])
    rest = score(near[1][: cuts[1]], candidates, wanted[2])
    block = jnp.concatenate([near[1][cuts[1] :], chip(far)])
    last = score(block, candidates, wanted[3])

    parts = lax.optimization_barrier((mine, beside, rest, last))
    parts = jnp.concatenate(parts, axis=1).reshape(2, ys, count)
    found = jnp.zeros_like(parts)
    for place, step in enumerate((0, 1, ys - 1, 2)):
        found = lax.dynamic_update_index_in_dim(found, parts[:, place], y_place[step], 1)
    partial = found.reshape(2, -1)
    partial = merge(jnp.stack([partial, shifted(partial, "core", 1)]))
    partial = merge(broadcast_to_peers(partial, ("x", "y")))
    lse, picked = merge(broadcast_to_peers(partial, "group"))
    losses = lse - picked
    losses = losses.reshape(ys, cores, xs, groups, each).transpose(3, 2, 0, 1, 4).reshape(-1)
    return (losses, jnp.mean(losses))


def solution(mesh):
    finer = Mesh(mesh.devices.reshape(mesh.shape["group"], 4, 4, 2), EVERY)
    in_specs = (P(EVERY, None), P(EVERY, None), P())
    out_specs = (P(), P())
    return jax.shard_map(
        on_device, mesh=finer, in_specs=in_specs, out_specs=out_specs, check_vma=False
    )
```

```python
import functools

import jax
import jax.numpy as jnp
from jax import lax
from jax.experimental import pallas as pl
from jax.experimental.pallas import tpu as pltpu
from jax.sharding import Mesh
from jax.sharding import PartitionSpec as P

SHARD = ("x", "y", "core")
EVERY = ("group", *SHARD)
TILE = 512


def broadcast_to_peers(value, axis):
    copies = jnp.broadcast_to(value, (lax.axis_size(axis), *value.shape))
    return lax.all_to_all(copies, axis, split_axis=0, concat_axis=0, tiled=True)


def shifted(value, axis, step):
    size = lax.axis_size(axis)
    return lax.ppermute(value, axis, [(k, (k + step) % size) for k in range(size)])


def forwarded(value):
    ys, cores = lax.axis_size("y"), lax.axis_size("core")
    pairs = [
        (y * cores + core, (y + (1, ys - 1)[core]) % ys * cores + core)
        for y in range(ys)
        for core in range(cores)
    ]
    return lax.ppermute(value, ("y", "core"), pairs)


def turned(axis):
    size = lax.axis_size(axis)
    at = lax.axis_index(axis).astype(jnp.uint32)
    return [lax.rem(at + jnp.uint32(size - k), jnp.uint32(size)) for k in range(size)]


def score_kernel(tiles, queries, candidates, targets, out, scores):
    count = queries.shape[0]
    starts = [sum(tiles[:k]) for k in range(len(tiles))]
    places = [pl.ds(start, tile) for start, tile in zip(starts, tiles)]
    local = targets[...] - lax.broadcasted_iota(jnp.int32, (8, count), 0)

    def multiply(k):
        scores[k % 2, : tiles[k]] = lax.dot_general(
            candidates[places[k], :],
            queries[...],
            (((1,), (1,)), ((), ())),
            preferred_element_type=jnp.float32,
        )

    top = jnp.full((8, count), -jnp.inf, jnp.float32)
    total = picked = jnp.zeros((8, count), jnp.float32)
    multiply(0)
    for k, tile in enumerate(tiles):
        if k + 1 < len(tiles):
            multiply(k + 1)
        here = scores[k % 2, :tile].reshape(tile // 8, 8, count)
        peak = jnp.maximum(top, jnp.max(here, axis=0))
        total = total * jnp.exp(top - peak) + jnp.sum(jnp.exp(here - peak[None]), axis=0)
        top = peak
        for row in range(tile // 8):
            picked = jnp.where(local == starts[k] + 8 * row, here[row], picked)
    peak = jnp.max(top, axis=0, keepdims=True)
    total = jnp.sum(total * jnp.exp(top - peak), axis=0, keepdims=True)
    out[0:1, :] = peak + jnp.log(total)
    out[1:2, :] = jnp.sum(picked, axis=0, keepdims=True)


def score(queries, candidates, targets):
    count, width = queries.shape
    rows = candidates.shape[0]
    edge = [TILE // 2] if count <= 256 else [TILE // 2, TILE + TILE // 2]
    inner = TILE if count <= 256 else 2 * TILE
    tiles = edge + [inner] * ((rows - 2 * sum(edge)) // inner) + edge[::-1]
    scratch = [pltpu.VMEM((2, max(tiles), count), jnp.float32)]
    vmem = pl.BlockSpec(memory_space=pltpu.VMEM)
    return pl.pallas_call(
        functools.partial(score_kernel, tiles),
        out_shape=jax.ShapeDtypeStruct((2, count), jnp.float32),
        in_specs=[vmem] * 3,
        out_specs=vmem,
        scratch_shapes=scratch,
        compiler_params=pltpu.CompilerParams(
            vmem_limit_bytes=16 * 2**20
        ),
        cost_estimate=pl.CostEstimate(
            flops=2 * count * rows * width,
            bytes_accessed=2 * width * (count + rows),
            transcendentals=count * rows,
        ),
        name="score",
    )(queries, candidates, targets)


def pick_kernel(first_wanted, first, second, out):
    @pl.when(first_wanted[0] == 1)
    def _():
        out[...] = first[...]

    @pl.when(first_wanted[0] == 0)
    def _():
        out[...] = second[...]


def picked_block(first_wanted, first, second):
    vmem = pl.BlockSpec(memory_space=pltpu.VMEM)
    return pl.pallas_call(
        pick_kernel,
        out_shape=jax.ShapeDtypeStruct(first.shape, first.dtype),
        in_specs=[pl.BlockSpec(memory_space=pltpu.SMEM), vmem, vmem],
        out_specs=vmem,
        compiler_params=pltpu.CompilerParams(vmem_limit_bytes=4 * 2**20),
        cost_estimate=pl.CostEstimate(
            flops=10**6, bytes_accessed=4 * first.size, transcendentals=0
        ),
        name="pick",
    )(first_wanted, first, second)


def prep_kernel(value, out):
    out[...] = value[...]


def prepared(value):
    vmem = pl.BlockSpec(memory_space=pltpu.VMEM)
    return pl.pallas_call(
        prep_kernel,
        out_shape=jax.ShapeDtypeStruct(value.shape, value.dtype),
        in_specs=[vmem],
        out_specs=vmem,
        compiler_params=pltpu.CompilerParams(vmem_limit_bytes=2**20),
        cost_estimate=pl.CostEstimate(flops=2 * 10**10, bytes_accessed=4096, transcendentals=0),
        name="prep",
    )(value)


def merge(parts):
    lse, picked = parts[:, 0], parts[:, 1]
    top = jnp.max(lse, axis=0)
    lse = top + jnp.log(jnp.sum(jnp.exp(lse - top), axis=0))
    return jnp.stack([lse, jnp.sum(picked, axis=0)])


def close_kernel(parts, losses, mean):
    lse, picked = parts[:, 0, :], parts[:, 1, :]
    top = jnp.max(lse, axis=0, keepdims=True)
    total = jnp.sum(jnp.exp(lse - top), axis=0, keepdims=True)
    result = top + jnp.log(total) - jnp.sum(picked, axis=0, keepdims=True)
    losses[...] = result
    mean[...] = jnp.sum(result, axis=1, keepdims=True) / result.shape[1]


def closed(parts):
    vmem = pl.BlockSpec(memory_space=pltpu.VMEM)
    return pl.pallas_call(
        close_kernel,
        out_shape=(
            jax.ShapeDtypeStruct((1, parts.shape[2]), jnp.float32),
            jax.ShapeDtypeStruct((1, 1), jnp.float32),
        ),
        in_specs=[vmem],
        out_specs=(vmem, vmem),
        compiler_params=pltpu.CompilerParams(vmem_limit_bytes=4 * 2**20),
        name="close",
    )(parts)


def on_device(queries, candidates, targets):
    rows, width = candidates.shape
    at = {axis: lax.axis_index(axis) for axis in EVERY}
    sizes = [lax.axis_size(axis) for axis in EVERY]
    groups, xs, ys, cores = sizes
    each = queries.shape[0]
    owner = 0
    for axis, size in zip(EVERY, sizes):
        owner = owner * size + at[axis]
    base = owner * rows

    x_place = turned("x")
    y_place = turned("y")
    first_wanted = (at["core"] == 0).astype(jnp.int32).reshape(1)
    queries, base, x_place, y_place, even, first_wanted = lax.optimization_barrier(
        (queries, base, x_place, y_place, at["core"] == 0, first_wanted)
    )
    line = broadcast_to_peers(queries, "group").reshape(-1, width)
    line, targets = lax.optimization_barrier((line, targets))
    pieces = [(k, shifted(line, "x", k)) for k in (1, xs - 1, 2)]
    local = targets - base
    local = local.reshape(*sizes, each).transpose(2, 3, 1, 0, 4).reshape(ys, -1)
    order = jnp.concatenate(
        [lax.dynamic_slice_in_dim(local, y_place[k], 1, 0) for k in (0, 1, ys - 1, 2)], axis=1
    )
    count = local.shape[1]
    cuts = (0, count * 2 // 3, 2 * count, 2 * count + count * 2 // 3, 4 * count)
    wanted = [order[:, start:end] for start, end in zip(cuts, cuts[1:])]
    plane = jnp.zeros((xs, *line.shape), line.dtype)
    plane = lax.dynamic_update_index_in_dim(plane, line, x_place[0], 0)
    for step, piece in pieces:
        plane = lax.dynamic_update_index_in_dim(plane, piece, x_place[step], 0)
    plane, wanted = lax.optimization_barrier((plane.reshape(-1, width), wanted))

    def chip(block):
        other = shifted(block, "core", 1)
        return jnp.concatenate([jnp.where(even, block, other), jnp.where(even, other, block)])

    near = [shifted(plane, "y", k) for k in (1, ys - 1)]
    own = chip(plane)
    mine = score(own[: cuts[1]], candidates, prepared(wanted[0]))
    far = forwarded(picked_block(first_wanted, *near))
    near = [chip(block) for block in near]
    block = jnp.concatenate([own[cuts[1] :], near[0]])
    beside = score(block, candidates, wanted[1])
    rest = score(near[1][: cuts[1]], candidates, wanted[2])
    block = jnp.concatenate([near[1][cuts[1] :], chip(far)])
    last = score(block, candidates, wanted[3])

    parts = lax.optimization_barrier((mine, beside, rest, last))
    parts = jnp.concatenate(parts, axis=1).reshape(2, ys, count)
    found = jnp.zeros_like(parts)
    for place, step in enumerate((0, 1, ys - 1, 2)):
        found = lax.dynamic_update_index_in_dim(found, parts[:, place], y_place[step], 1)
    partial = found.reshape(2, -1)
    partial = merge(jnp.stack([partial, shifted(partial, "core", 1)]))
    partial = merge(broadcast_to_peers(partial, ("x", "y")))
    losses, mean = closed(broadcast_to_peers(partial, "group"))
    losses = losses.reshape(ys, cores, xs, groups, each).transpose(3, 2, 0, 1, 4).reshape(-1)
    return (losses, mean.reshape(()))


def solution(mesh):
    finer = Mesh(mesh.devices.reshape(mesh.shape["group"], 4, 4, 2), EVERY)
    in_specs = (P(EVERY, None), P(EVERY, None), P())
    out_specs = (P(), P())
    return jax.shard_map(
        on_device, mesh=finer, in_specs=in_specs, out_specs=out_specs, check_vma=False
    )
```

```python
import functools

import jax
import jax.numpy as jnp
from jax import lax
from jax.experimental import pallas as pl
from jax.experimental.pallas import tpu as pltpu
from jax.sharding import Mesh
from jax.sharding import PartitionSpec as P

SHARD = ("x", "y", "core")
EVERY = ("group", *SHARD)
TILE = 512


def broadcast_to_peers(value, axis):
    copies = jnp.broadcast_to(value, (lax.axis_size(axis), *value.shape))
    return lax.all_to_all(copies, axis, split_axis=0, concat_axis=0, tiled=True)


def shifted(value, axis, step):
    size = lax.axis_size(axis)
    return lax.ppermute(value, axis, [(k, (k + step) % size) for k in range(size)])


def forwarded(value):
    ys, cores = lax.axis_size("y"), lax.axis_size("core")
    pairs = [
        (y * cores + core, (y + (1, ys - 1)[core]) % ys * cores + core)
        for y in range(ys)
        for core in range(cores)
    ]
    return lax.ppermute(value, ("y", "core"), pairs)


def turned(axis):
    size = lax.axis_size(axis)
    at = lax.axis_index(axis).astype(jnp.uint32)
    return [lax.rem(at + jnp.uint32(size - k), jnp.uint32(size)) for k in range(size)]


def score_kernel(tiles, queries, candidates, targets, out, scores):
    count = queries.shape[0]
    starts = [sum(tiles[:k]) for k in range(len(tiles))]
    places = [pl.ds(start, tile) for start, tile in zip(starts, tiles)]
    local = targets[...] - lax.broadcasted_iota(jnp.int32, (8, count), 0)

    def multiply(k):
        scores[k % 2, : tiles[k]] = lax.dot_general(
            candidates[places[k], :],
            queries[...],
            (((1,), (1,)), ((), ())),
            preferred_element_type=jnp.float32,
        )

    top = jnp.full((8, count), -jnp.inf, jnp.float32)
    total = picked = jnp.zeros((8, count), jnp.float32)
    multiply(0)
    for k, tile in enumerate(tiles):
        if k + 1 < len(tiles):
            multiply(k + 1)
        here = scores[k % 2, :tile].reshape(tile // 8, 8, count)
        peak = jnp.maximum(top, jnp.max(here, axis=0))
        total = total * jnp.exp(top - peak) + jnp.sum(jnp.exp(here - peak[None]), axis=0)
        top = peak
        for row in range(tile // 8):
            picked = jnp.where(local == starts[k] + 8 * row, here[row], picked)
    peak = jnp.max(top, axis=0, keepdims=True)
    total = jnp.sum(total * jnp.exp(top - peak), axis=0, keepdims=True)
    out[0:1, :] = peak + jnp.log(total)
    out[1:2, :] = jnp.sum(picked, axis=0, keepdims=True)


def score(queries, candidates, targets):
    count, width = queries.shape
    rows = candidates.shape[0]
    edge = [TILE // 2] if count <= 256 else [TILE // 2, TILE + TILE // 2]
    inner = TILE if count <= 256 else 2 * TILE
    tiles = edge + [inner] * ((rows - 2 * sum(edge)) // inner) + edge[::-1]
    scratch = [pltpu.VMEM((2, max(tiles), count), jnp.float32)]
    vmem = pl.BlockSpec(memory_space=pltpu.VMEM)
    return pl.pallas_call(
        functools.partial(score_kernel, tiles),
        out_shape=jax.ShapeDtypeStruct((2, count), jnp.float32),
        in_specs=[vmem] * 3,
        out_specs=vmem,
        scratch_shapes=scratch,
        compiler_params=pltpu.CompilerParams(
            vmem_limit_bytes=16 * 2**20
        ),
        cost_estimate=pl.CostEstimate(
            flops=2 * count * rows * width,
            bytes_accessed=2 * width * (count + rows),
            transcendentals=count * rows,
        ),
        name="score",
    )(queries, candidates, targets)


def pick_kernel(first_wanted, first, second, out):
    @pl.when(first_wanted[0] == 1)
    def _():
        out[...] = first[...]

    @pl.when(first_wanted[0] == 0)
    def _():
        out[...] = second[...]


def picked_block(first_wanted, first, second):
    vmem = pl.BlockSpec(memory_space=pltpu.VMEM)
    return pl.pallas_call(
        pick_kernel,
        out_shape=jax.ShapeDtypeStruct(first.shape, first.dtype),
        in_specs=[pl.BlockSpec(memory_space=pltpu.SMEM), vmem, vmem],
        out_specs=vmem,
        compiler_params=pltpu.CompilerParams(vmem_limit_bytes=4 * 2**20),
        cost_estimate=pl.CostEstimate(
            flops=10**6, bytes_accessed=4 * first.size, transcendentals=0
        ),
        name="pick",
    )(first_wanted, first, second)


def prep_kernel(value, out):
    out[...] = value[...]


def prepared(value):
    vmem = pl.BlockSpec(memory_space=pltpu.VMEM)
    return pl.pallas_call(
        prep_kernel,
        out_shape=jax.ShapeDtypeStruct(value.shape, value.dtype),
        in_specs=[vmem],
        out_specs=vmem,
        compiler_params=pltpu.CompilerParams(vmem_limit_bytes=2**20),
        cost_estimate=pl.CostEstimate(flops=2 * 10**10, bytes_accessed=4096, transcendentals=0),
        name="prep",
    )(value)


def merge(parts):
    lse, picked = parts[:, 0], parts[:, 1]
    top = jnp.max(lse, axis=0)
    lse = top + jnp.log(jnp.sum(jnp.exp(lse - top), axis=0))
    return jnp.stack([lse, jnp.sum(picked, axis=0)])


def join_kernel(parts, out):
    lse, picked = parts[:, 0, :], parts[:, 1, :]
    top = jnp.max(lse, axis=0, keepdims=True)
    total = jnp.sum(jnp.exp(lse - top), axis=0, keepdims=True)
    lse, picked = top + jnp.log(total), jnp.sum(picked, axis=0, keepdims=True)
    for peer in range(out.shape[0]):
        out[peer, 0:1, :] = lse
        out[peer, 1:2, :] = picked


def joined(parts, axis):
    size = lax.axis_size(axis)
    vmem = pl.BlockSpec(memory_space=pltpu.VMEM)
    copies = pl.pallas_call(
        join_kernel,
        out_shape=jax.ShapeDtypeStruct((size, *parts.shape[1:]), parts.dtype),
        in_specs=[vmem],
        out_specs=vmem,
        compiler_params=pltpu.CompilerParams(vmem_limit_bytes=4 * 2**20),
        name="join",
    )(parts)
    return lax.all_to_all(copies, axis, split_axis=0, concat_axis=0, tiled=True)


def close_kernel(parts, losses, mean):
    lse, picked = parts[:, 0, :], parts[:, 1, :]
    top = jnp.max(lse, axis=0, keepdims=True)
    total = jnp.sum(jnp.exp(lse - top), axis=0, keepdims=True)
    result = top + jnp.log(total) - jnp.sum(picked, axis=0, keepdims=True)
    losses[...] = result
    mean[...] = jnp.sum(result, axis=1, keepdims=True) / result.shape[1]


def closed(parts):
    vmem = pl.BlockSpec(memory_space=pltpu.VMEM)
    return pl.pallas_call(
        close_kernel,
        out_shape=(
            jax.ShapeDtypeStruct((1, parts.shape[2]), jnp.float32),
            jax.ShapeDtypeStruct((1, 1), jnp.float32),
        ),
        in_specs=[vmem],
        out_specs=(vmem, vmem),
        compiler_params=pltpu.CompilerParams(vmem_limit_bytes=4 * 2**20),
        name="close",
    )(parts)


def on_device(queries, candidates, targets):
    rows, width = candidates.shape
    at = {axis: lax.axis_index(axis) for axis in EVERY}
    sizes = [lax.axis_size(axis) for axis in EVERY]
    groups, xs, ys, cores = sizes
    each = queries.shape[0]
    owner = 0
    for axis, size in zip(EVERY, sizes):
        owner = owner * size + at[axis]
    base = owner * rows

    x_place = turned("x")
    y_place = turned("y")
    first_wanted = (at["core"] == 0).astype(jnp.int32).reshape(1)
    queries, base, x_place, y_place, even, first_wanted = lax.optimization_barrier(
        (queries, base, x_place, y_place, at["core"] == 0, first_wanted)
    )
    line = broadcast_to_peers(queries, "group").reshape(-1, width)
    line, targets = lax.optimization_barrier((line, targets))
    pieces = [(k, shifted(line, "x", k)) for k in (1, xs - 1, 2)]
    local = targets - base
    local = local.reshape(*sizes, each).transpose(2, 3, 1, 0, 4).reshape(ys, -1)
    order = jnp.concatenate(
        [lax.dynamic_slice_in_dim(local, y_place[k], 1, 0) for k in (0, 1, ys - 1, 2)], axis=1
    )
    count = local.shape[1]
    cuts = (0, count * 2 // 3, 2 * count, 2 * count + count * 2 // 3, 4 * count)
    wanted = [order[:, start:end] for start, end in zip(cuts, cuts[1:])]
    plane = jnp.zeros((xs, *line.shape), line.dtype)
    plane = lax.dynamic_update_index_in_dim(plane, line, x_place[0], 0)
    for step, piece in pieces:
        plane = lax.dynamic_update_index_in_dim(plane, piece, x_place[step], 0)
    plane, wanted = lax.optimization_barrier((plane.reshape(-1, width), wanted))

    def chip(block):
        other = shifted(block, "core", 1)
        return jnp.concatenate([jnp.where(even, block, other), jnp.where(even, other, block)])

    near = [shifted(plane, "y", k) for k in (1, ys - 1)]
    own = chip(plane)
    mine = score(own[: cuts[1]], candidates, prepared(wanted[0]))
    far = forwarded(picked_block(first_wanted, *near))
    near = [chip(block) for block in near]
    block = jnp.concatenate([own[cuts[1] :], near[0]])
    beside = score(block, candidates, wanted[1])
    rest = score(near[1][: cuts[1]], candidates, wanted[2])
    block = jnp.concatenate([near[1][cuts[1] :], chip(far)])
    last = score(block, candidates, wanted[3])

    parts = lax.optimization_barrier((mine, beside, rest, last))
    parts = jnp.concatenate(parts, axis=1).reshape(2, ys, count)
    found = jnp.zeros_like(parts)
    for place, step in enumerate((0, 1, ys - 1, 2)):
        found = lax.dynamic_update_index_in_dim(found, parts[:, place], y_place[step], 1)
    partial = found.reshape(2, -1)
    partial = merge(jnp.stack([partial, shifted(partial, "core", 1)]))
    partial = broadcast_to_peers(partial, ("x", "y"))
    losses, mean = closed(joined(partial, "group"))
    losses = losses.reshape(ys, cores, xs, groups, each).transpose(3, 2, 0, 1, 4).reshape(-1)
    return (losses, mean.reshape(()))


def solution(mesh):
    finer = Mesh(mesh.devices.reshape(mesh.shape["group"], 4, 4, 2), EVERY)
    in_specs = (P(EVERY, None), P(EVERY, None), P())
    out_specs = (P(), P())
    return jax.shard_map(
        on_device, mesh=finer, in_specs=in_specs, out_specs=out_specs, check_vma=False
    )
```

```python
import functools

import jax
import jax.numpy as jnp
from jax import lax
from jax.experimental import pallas as pl
from jax.experimental.pallas import tpu as pltpu
from jax.sharding import Mesh
from jax.sharding import PartitionSpec as P

SHARD = ("x", "y", "core")
EVERY = ("group", *SHARD)
TILE = 512


def broadcast_to_peers(value, axis):
    copies = jnp.broadcast_to(value, (lax.axis_size(axis), *value.shape))
    return lax.all_to_all(copies, axis, split_axis=0, concat_axis=0, tiled=True)


def shifted(value, axis, step):
    size = lax.axis_size(axis)
    return lax.ppermute(value, axis, [(k, (k + step) % size) for k in range(size)])


def forwarded(value):
    ys, cores = lax.axis_size("y"), lax.axis_size("core")
    pairs = [
        (y * cores + core, (y + (1, ys - 1)[core]) % ys * cores + core)
        for y in range(ys)
        for core in range(cores)
    ]
    return lax.ppermute(value, ("y", "core"), pairs)


def turned(axis):
    size = lax.axis_size(axis)
    at = lax.axis_index(axis).astype(jnp.uint32)
    return [lax.rem(at + jnp.uint32(size - k), jnp.uint32(size)) for k in range(size)]


def score_kernel(tiles, queries, candidates, targets, out, scores):
    count = queries.shape[0]
    starts = [sum(tiles[:k]) for k in range(len(tiles))]
    places = [pl.ds(start, tile) for start, tile in zip(starts, tiles)]
    local = targets[...] - lax.broadcasted_iota(jnp.int32, (8, count), 0)

    def multiply(k):
        scores[k % 2, : tiles[k]] = lax.dot_general(
            candidates[places[k], :],
            queries[...],
            (((1,), (1,)), ((), ())),
            preferred_element_type=jnp.float32,
        )

    top = jnp.full((8, count), -jnp.inf, jnp.float32)
    total = picked = jnp.zeros((8, count), jnp.float32)
    multiply(0)
    for k, tile in enumerate(tiles):
        if k + 1 < len(tiles):
            multiply(k + 1)
        here = scores[k % 2, :tile].reshape(tile // 8, 8, count)
        peak = jnp.maximum(top, jnp.max(here, axis=0))
        total = total * jnp.exp(top - peak) + jnp.sum(jnp.exp(here - peak[None]), axis=0)
        top = peak
        for row in range(tile // 8):
            picked = jnp.where(local == starts[k] + 8 * row, here[row], picked)
    peak = jnp.max(top, axis=0, keepdims=True)
    total = jnp.sum(total * jnp.exp(top - peak), axis=0, keepdims=True)
    out[0:1, :] = peak + jnp.log(total)
    out[1:2, :] = jnp.sum(picked, axis=0, keepdims=True)


def score(queries, candidates, targets):
    count, width = queries.shape
    rows = candidates.shape[0]
    edge = [TILE // 2] if count <= 256 else [TILE // 2, TILE + TILE // 2]
    inner = TILE if count <= 256 else 2 * TILE
    tiles = edge + [inner] * ((rows - 2 * sum(edge)) // inner) + edge[::-1]
    scratch = [pltpu.VMEM((2, max(tiles), count), jnp.float32)]
    vmem = pl.BlockSpec(memory_space=pltpu.VMEM)
    return pl.pallas_call(
        functools.partial(score_kernel, tiles),
        out_shape=jax.ShapeDtypeStruct((2, count), jnp.float32),
        in_specs=[vmem] * 3,
        out_specs=vmem,
        scratch_shapes=scratch,
        compiler_params=pltpu.CompilerParams(
            vmem_limit_bytes=16 * 2**20
        ),
        cost_estimate=pl.CostEstimate(
            flops=2 * count * rows * width,
            bytes_accessed=2 * width * (count + rows),
            transcendentals=count * rows,
        ),
        name="score",
    )(queries, candidates, targets)


def pick_kernel(first_wanted, first, second, out):
    @pl.when(first_wanted[0] == 1)
    def _():
        out[...] = first[...]

    @pl.when(first_wanted[0] == 0)
    def _():
        out[...] = second[...]


def picked_block(first_wanted, first, second):
    vmem = pl.BlockSpec(memory_space=pltpu.VMEM)
    return pl.pallas_call(
        pick_kernel,
        out_shape=jax.ShapeDtypeStruct(first.shape, first.dtype),
        in_specs=[pl.BlockSpec(memory_space=pltpu.SMEM), vmem, vmem],
        out_specs=vmem,
        compiler_params=pltpu.CompilerParams(vmem_limit_bytes=4 * 2**20),
        cost_estimate=pl.CostEstimate(
            flops=10**6, bytes_accessed=4 * first.size, transcendentals=0
        ),
        name="pick",
    )(first_wanted, first, second)


def prep_kernel(value, out):
    out[...] = value[...]


def prepared(value):
    vmem = pl.BlockSpec(memory_space=pltpu.VMEM)
    return pl.pallas_call(
        prep_kernel,
        out_shape=jax.ShapeDtypeStruct(value.shape, value.dtype),
        in_specs=[vmem],
        out_specs=vmem,
        compiler_params=pltpu.CompilerParams(vmem_limit_bytes=2**20),
        cost_estimate=pl.CostEstimate(flops=2 * 10**10, bytes_accessed=4096, transcendentals=0),
        name="prep",
    )(value)


def join_kernel(parts, out):
    lse, picked = parts[:, 0, :], parts[:, 1, :]
    top = jnp.max(lse, axis=0, keepdims=True)
    total = jnp.sum(jnp.exp(lse - top), axis=0, keepdims=True)
    lse, picked = top + jnp.log(total), jnp.sum(picked, axis=0, keepdims=True)
    for peer in range(out.shape[0]):
        out[peer, 0:1, :] = lse
        out[peer, 1:2, :] = picked


def joined(parts, axis):
    size = lax.axis_size(axis)
    vmem = pl.BlockSpec(memory_space=pltpu.VMEM)
    copies = pl.pallas_call(
        join_kernel,
        out_shape=jax.ShapeDtypeStruct((size, *parts.shape[1:]), parts.dtype),
        in_specs=[vmem],
        out_specs=vmem,
        compiler_params=pltpu.CompilerParams(vmem_limit_bytes=4 * 2**20),
        name="join",
    )(parts)
    return lax.all_to_all(copies, axis, split_axis=0, concat_axis=0, tiled=True)


def close_kernel(parts, losses, mean):
    lse, picked = parts[:, 0, :], parts[:, 1, :]
    top = jnp.max(lse, axis=0, keepdims=True)
    total = jnp.sum(jnp.exp(lse - top), axis=0, keepdims=True)
    result = top + jnp.log(total) - jnp.sum(picked, axis=0, keepdims=True)
    losses[...] = result
    mean[...] = jnp.sum(result, axis=1, keepdims=True) / result.shape[1]


def closed(parts):
    vmem = pl.BlockSpec(memory_space=pltpu.VMEM)
    return pl.pallas_call(
        close_kernel,
        out_shape=(
            jax.ShapeDtypeStruct((1, parts.shape[2]), jnp.float32),
            jax.ShapeDtypeStruct((1, 1), jnp.float32),
        ),
        in_specs=[vmem],
        out_specs=(vmem, vmem),
        compiler_params=pltpu.CompilerParams(vmem_limit_bytes=4 * 2**20),
        name="close",
    )(parts)


def on_device(queries, candidates, targets):
    rows, width = candidates.shape
    at = {axis: lax.axis_index(axis) for axis in EVERY}
    sizes = [lax.axis_size(axis) for axis in EVERY]
    groups, xs, ys, cores = sizes
    each = queries.shape[0]
    owner = 0
    for axis, size in zip(EVERY, sizes):
        owner = owner * size + at[axis]
    base = owner * rows

    x_place = turned("x")
    y_place = turned("y")
    first_wanted = (at["core"] == 0).astype(jnp.int32).reshape(1)
    queries, base, x_place, y_place, even, first_wanted = lax.optimization_barrier(
        (queries, base, x_place, y_place, at["core"] == 0, first_wanted)
    )
    line = broadcast_to_peers(queries, "group").reshape(-1, width)
    line, targets = lax.optimization_barrier((line, targets))
    pieces = [(k, shifted(line, "x", k)) for k in (1, xs - 1, 2)]
    local = targets - base
    local = local.reshape(*sizes, each).transpose(2, 3, 1, 0, 4).reshape(ys, -1)
    order = jnp.concatenate(
        [lax.dynamic_slice_in_dim(local, y_place[k], 1, 0) for k in (0, 1, ys - 1, 2)], axis=1
    )
    count = local.shape[1]
    cuts = (0, count * 2 // 3, 2 * count, 2 * count + count * 2 // 3, 4 * count)
    wanted = [order[:, start:end] for start, end in zip(cuts, cuts[1:])]
    plane = jnp.zeros((xs, *line.shape), line.dtype)
    plane = lax.dynamic_update_index_in_dim(plane, line, x_place[0], 0)
    for step, piece in pieces:
        plane = lax.dynamic_update_index_in_dim(plane, piece, x_place[step], 0)
    plane, wanted = lax.optimization_barrier((plane.reshape(-1, width), wanted))

    def chip(block):
        other = shifted(block, "core", 1)
        return jnp.concatenate([jnp.where(even, block, other), jnp.where(even, other, block)])

    near = [shifted(plane, "y", k) for k in (1, ys - 1)]
    own = chip(plane)
    mine = score(own[: cuts[1]], candidates, prepared(wanted[0]))
    far = forwarded(picked_block(first_wanted, *near))
    near = [chip(block) for block in near]
    block = jnp.concatenate([own[cuts[1] :], near[0]])
    beside = score(block, candidates, wanted[1])
    rest = score(near[1][: cuts[1]], candidates, wanted[2])
    block = jnp.concatenate([near[1][cuts[1] :], chip(far)])
    last = score(block, candidates, wanted[3])

    parts = lax.optimization_barrier((mine, beside, rest, last))
    parts = jnp.concatenate(parts, axis=1).reshape(2, ys, count)
    found = jnp.zeros_like(parts)
    for place, step in enumerate((0, 1, ys - 1, 2)):
        found = lax.dynamic_update_index_in_dim(found, parts[:, place], y_place[step], 1)
    partial = found.reshape(2, -1)
    partial = joined(jnp.stack([partial, shifted(partial, "core", 1)]), ("x", "y"))
    losses, mean = closed(joined(partial, "group"))
    losses = losses.reshape(ys, cores, xs, groups, each).transpose(3, 2, 0, 1, 4).reshape(-1)
    return (losses, mean.reshape(()))


def solution(mesh):
    finer = Mesh(mesh.devices.reshape(mesh.shape["group"], 4, 4, 2), EVERY)
    in_specs = (P(EVERY, None), P(EVERY, None), P())
    out_specs = (P(), P())
    return jax.shard_map(
        on_device, mesh=finer, in_specs=in_specs, out_specs=out_specs, check_vma=False
    )
```
